32 devices in a mesh: comp: 8 (over z, x), vocab: 4 (over y, core).
Axes of the slice: x: 2, y: 2, z: 4, core: 2. Of those that a mesh axis runs over, the one named last changes fastest.
Arguments:
- hidden: bfloat16 [512, 2048], P('comp'), may hold values from -6 to 6
- routes: int32 [512, 4], P('comp'), may hold values from 0 to 15, all different within a row; in each aligned block of 64 rows (0 to 63, 64 to 127, ...) at most 32 rows name the same one
- targets: int32 [512], P('comp'), may hold values from 0 to 8191
- saved_lse: float32 [512, 4], P('comp'), as said below
- target_logprob: float32 [512, 4], P('comp'), may hold values from -8 to -4
- prior_weight: bfloat16 [2048, 16], P('vocab'), may hold values from -0.25 to 0.25
- projection: bfloat16 [16, 2048, 2048], P('comp', None, 'vocab'), as said below
- embedding: bfloat16 [2048, 8192], P(None, 'vocab'), as said below
Outputs:
- grad_hidden: float32 [512, 2048], P('comp', 'vocab')
- grad_prior: float32 [2048, 16], P('vocab')
- grad_projection: bfloat16 [16, 2048, 2048], P('comp', None, 'vocab')
- grad_embedding: bfloat16 [2048, 8192], P('comp', 'vocab')
The draws below stay inside these ranges and needn't reach their ends.
Inputs may be any that keep to these rules, and one draw needn't show every extreme that they name: `routes`: in each aligned block of 64 rows (the tokens of one index of comp) the 4 entries of a row differ, and no component is named by more than 32 rows; some component reaches 32 in some block. `projection`: entries lie within 4 / sqrt(2048) of zero. `embedding`: entries lie within 6.5 / sqrt(2048) of zero. `saved_lse`: each entry lies between ln(8192) - 2.7 and ln(8192) - 0.9.
All inputs are finite; a program needn't handle non-finite values.
Results may differ from the reference program's by a relative error of at most 0.0056.
Values may be sent and summed in bfloat16 or wider, within the bound.
A program may use at most 128 MiB of HBM per device.

```python
import math
import jax
import jax.numpy as jnp
import numpy as np
from jax import lax

D = 2048
TOP = 4
TOK_DEV = 64
VOCAB = 8192
COMPONENTS = 16
TOKENS = 512
CAP = 32
N_COMP = 8


def draw_hidden(key, part):
    own_key = jax.random.fold_in(key, 12)
    values = jnp.clip(jax.random.normal(own_key, (TOKENS, D), jnp.float32), -6.0, 6.0)
    return values.astype(jnp.bfloat16)


def draw_projection(key, part):
    own_key = jax.random.fold_in(key, 22)
    factor = 1.0 / jnp.sqrt(jnp.float32(D))
    values = jnp.clip(jax.random.normal(own_key, (COMPONENTS, D, D), jnp.float32), -4.0, 4.0) * factor
    return values.astype(jnp.bfloat16)


def draw_embedding(key, part):
    own_key = jax.random.fold_in(key, 31)
    factor = 1.6 / jnp.sqrt(jnp.float32(D))
    values = jnp.clip(jax.random.normal(own_key, (D, VOCAB), jnp.float32), -4.0, 4.0) * factor
    return values.astype(jnp.bfloat16)


def draw_saved_lse(key, part):
    own_key = jax.random.fold_in(key, 41)
    center = jnp.log(jnp.float32(VOCAB)) + 0.5
    offset = jax.random.uniform(own_key, (TOKENS, TOP), jnp.float32, 1.6, 3.0)
    return (center - offset).astype(jnp.float32)


def plant(values, key, smallest, largest):
    longest = values.shape.index(max(values.shape))
    spots = []
    for shift in (0, 1):
        where = [jax.random.randint(jax.random.fold_in(key, axis), (), 0, length) for axis, length in enumerate(values.shape)]
        where[longest] = (where[longest] + shift) % values.shape[longest]
        spots.append(tuple(where))
    return values.at[spots[0]].set(smallest).at[spots[1]].set(largest)


def steps_of(stream_key, shape, pieces, least, top_value):
    def one(dim, parts):
        steps = jax.random.uniform(jax.random.fold_in(jax.random.fold_in(stream_key, 6), dim), (parts,), jnp.float32, least / len(pieces), top_value / len(pieces))
        return jnp.repeat(jnp.exp(steps), shape[dim] // parts).reshape((-1,) + (1,) * (len(shape) - dim - 1))

    gain = one(*pieces[0])
    for cut in pieces[1:]:
        gain = gain * one(*cut)
    return gain


def deal_out(rng, own, number, rows, number_of, top, limit, slope):
    ranking = jax.random.permutation(rng, number_of)
    heavy_load, common = portions_of(number_of, rows * top, limit, slope, True), portions_of(number_of, rows * top, limit, slope, False)
    places = jnp.arange(number_of)

    def named(tallies, rotation):
        used = int((tallies > 0).sum())
        fixed = max(1, used // 4)
        moved = fixed + (places - fixed + rotation * (used - fixed)) % max(1, number_of - fixed)
        return jnp.zeros((number_of,), jnp.int32).at[ranking[jnp.where(places < fixed, places, moved)]].set(jnp.asarray(tallies, jnp.int32))

    tallies = jnp.where(number % 4 == 0, named(heavy_load, number // 4), named(common, number - number // 4 - 1))
    mixed = jax.random.permutation(jax.random.fold_in(own, 3), number_of)
    giver, taker = mixed[0:number_of // 2 * 2:2], mixed[1:number_of // 2 * 2:2]
    margin = jnp.minimum(tallies[giver] - 1, limit - tallies[taker]) // 2
    margin = jnp.where((giver == ranking[0]) | (taker == ranking[0]) | (tallies[taker] == 0), 0, jnp.maximum(margin, 0))
    moved = jax.random.randint(jax.random.fold_in(own, 4), (number_of // 2,), 0, 1 << 20) % (margin + 1)
    tallies = tallies.at[giver].add(-moved).at[taker].add(moved)
    labels = jnp.searchsorted(jnp.cumsum(tallies), jnp.arange(rows * top), side="right").astype(jnp.int32)
    grid = labels.reshape(top, rows).T
    grid = grid[jax.random.permutation(jax.random.fold_in(own, 1), rows)]
    rotation = jax.random.randint(jax.random.fold_in(own, 2), (rows, 1), 0, top)
    return jnp.take_along_axis(grid, (jnp.arange(top)[None, :] + rotation) % top, axis=1)


def portions_of(count, total, bound, lean, full):
    weights = [(1 << 20) // math.isqrt(rank ** lean) + 1 for rank in range(1, count + 1)]
    largest = bound if full else min(bound, max(-(-total // count), total * weights[0] // sum(weights)))
    least = 1 if total - largest >= count - 1 else 0
    holding, surplus = [largest] + [least] * (count - 1), total - largest - least * (count - 1)
    while surplus > 0:
        candidates = [i for i in range(1, count) if holding[i] < largest] or [i for i in range(1, count) if holding[i] < bound]
        pool, left = sum([weights[i] for i in candidates]), surplus
        for i in candidates:
            more = min(bound - holding[i], max(1, left * weights[i] // pool), surplus)
            holding[i] = holding[i] + more
            surplus = surplus - more
    return np.array(holding)


def noise(stream_key, dims, scale, most, split=(), kind=jnp.bfloat16):
    drawn = jax.random.normal(stream_key, dims, jnp.float32) * scale
    if len(split) > 0:
        drawn = steps_of(stream_key, dims, split, -0.22, 0.18) * drawn
    return jnp.clip(drawn, min=-most, max=most).astype(kind)


def setup_inputs(seed: int = 0) -> dict:
    key_list = jax.random.split(jax.random.key(seed), 9)
    hidden = draw_hidden(jax.random.fold_in(key_list[8], 71), 0)
    routes_keys = jax.random.split(jax.random.fold_in(key_list[1], 1), TOKENS // TOK_DEV)
    routes_turns = jax.random.permutation(jax.random.fold_in(key_list[1], 3), TOKENS // TOK_DEV)
    routes = jax.vmap(lambda own, number: deal_out(jax.random.fold_in(key_list[1], 2), own, number, TOK_DEV, COMPONENTS, TOP, CAP, 2))(routes_keys, routes_turns).reshape((TOKENS, TOP))
    targets = plant(jax.random.randint(key_list[2], (TOKENS,), 0, VOCAB), jax.random.fold_in(key_list[2], 1), 0, VOCAB - 1).astype(jnp.int32)
    saved_lse = draw_saved_lse(jax.random.fold_in(key_list[8], 71), 0)
    target_logprob = jnp.clip(-8.0 + 4.0 * jax.random.uniform(key_list[4], (TOKENS, TOP), jnp.float32) ** steps_of(key_list[4], (TOKENS, TOP), ((0, 8),), -0.2, 0.2), -8.0, -4.0)
    prior_weight = noise(key_list[5], (D, COMPONENTS), (D // 4) ** -0.5, 0.25, ((0, 4),))
    projection = draw_projection(jax.random.fold_in(key_list[8], 71), 0)
    embedding = draw_embedding(jax.random.fold_in(key_list[8], 71), 0)
    return {"hidden": hidden, "routes": routes, "targets": targets, "saved_lse": saved_lse, "target_logprob": target_logprob, "prior_weight": prior_weight, "projection": projection, "embedding": embedding}


def reference(hidden, routes, targets, saved_lse, target_logprob, prior_weight, projection, embedding):
    highest = lax.Precision.HIGHEST
    prior_logits = jnp.dot(hidden, prior_weight, preferred_element_type=jnp.float32)
    selected = jnp.take_along_axis(prior_logits, routes, axis=1)
    gate_weights = jax.nn.softmax(selected, axis=-1)
    posterior = jax.nn.softmax(jax.nn.log_softmax(selected, axis=-1) + target_logprob, axis=-1)
    picked = (routes[:, :, None] == jnp.arange(COMPONENTS, dtype=jnp.int32)[None, None, :]).astype(jnp.float32)
    prior_grads = jnp.sum((gate_weights - posterior)[:, :, None] * picked, axis=1)
    grad_prior = jnp.dot(hidden.astype(jnp.float32).T, prior_grads, precision=highest)
    prior_back = jnp.dot(prior_grads, prior_weight.astype(jnp.float32).T, precision=highest)

    slot_rows = N_COMP * CAP
    pair_comp = routes.reshape(N_COMP, TOK_DEV * TOP).astype(jnp.int32)
    pair_onehot = (pair_comp[:, :, None] == jnp.arange(COMPONENTS, dtype=jnp.int32)[None, None, :]).astype(jnp.int32)
    earlier = (jnp.cumsum(pair_onehot, axis=1) - pair_onehot).astype(jnp.int32)
    pair_rank = jnp.sum(earlier * pair_onehot, axis=2).astype(jnp.int32)
    block_ids = jnp.arange(N_COMP, dtype=jnp.int32)[:, None]
    position = (pair_comp * slot_rows + block_ids * CAP + pair_rank).reshape(-1).astype(jnp.int32)
    pair_token = jnp.repeat(jnp.arange(TOKENS, dtype=jnp.int32), TOP)
    slot_total = COMPONENTS * slot_rows
    rows_all = jnp.zeros((slot_total, D), hidden.dtype).at[position].set(hidden[pair_token])
    post_all = jnp.zeros((slot_total,), jnp.float32).at[position].set(posterior.reshape(-1))
    lse_all = jnp.zeros((slot_total,), jnp.float32).at[position].set(saved_lse.reshape(-1))
    target_all = jnp.zeros((slot_total,), jnp.int32).at[position].set(targets[pair_token].astype(jnp.int32))
    vocab_ids = jnp.arange(VOCAB, dtype=jnp.int32)

    def component(running, inputs):
        slot_input, weight, post_rows, lse_rows, target_rows = inputs
        preact = jnp.dot(slot_input, weight, preferred_element_type=jnp.float32)
        tanh_value = jnp.tanh(preact)
        z_rows = tanh_value.astype(jnp.bfloat16)
        logits = jnp.dot(z_rows, embedding, preferred_element_type=jnp.float32)
        target_hit = (target_rows[:, None] == vocab_ids[None, :]).astype(jnp.float32)
        logit_grads = (post_rows[:, None] * (jnp.exp(logits - lse_rows[:, None]) - target_hit)).astype(jnp.bfloat16)
        feature_grads = lax.dot_general(logit_grads, embedding, (((1,), (1,)), ((), ())), preferred_element_type=jnp.float32)
        pre_grads = (feature_grads * (1.0 - tanh_value * tanh_value)).astype(jnp.bfloat16)
        grad_weight = lax.dot_general(slot_input, pre_grads, (((0,), (0,)), ((), ())), preferred_element_type=jnp.float32).astype(jnp.bfloat16)
        slot_grads = lax.dot_general(pre_grads, weight, (((1,), (1,)), ((), ())), preferred_element_type=jnp.float32)
        embed_part = lax.dot_general(z_rows, logit_grads, (((0,), (0,)), ((), ())), preferred_element_type=jnp.float32)
        return running + embed_part, (grad_weight, slot_grads)

    start_sum = jnp.zeros((D, VOCAB), jnp.float32)
    inputs = (rows_all.reshape(COMPONENTS, slot_rows, D), projection, post_all.reshape(COMPONENTS, slot_rows),
              lse_all.reshape(COMPONENTS, slot_rows), target_all.reshape(COMPONENTS, slot_rows))
    embed_sum, (grad_projection, slot_grads) = lax.scan(component, start_sum, inputs)
    pair_grads = slot_grads.reshape(slot_total, D)[position].reshape(TOKENS, TOP, D)
    grad_hidden = jnp.sum(pair_grads, axis=1) + prior_back
    return grad_hidden, grad_prior, grad_projection, embed_sum.astype(jnp.bfloat16)
```

```python
import jax
import jax.numpy as jnp
from jax import lax
from jax.sharding import PartitionSpec as P


def core_swap(value, count):
    return lax.ppermute(value, "vocab", [(i, i ^ 1) for i in range(count)])


def vocab_gather(block, count):
    me = lax.axis_index("vocab")
    pairs = count // 2
    ring = [(i, (i + 2) % count) for i in range(count)]
    held = [block]
    for _ in range(pairs - 1):
        held.append(lax.ppermute(held[-1], "vocab", ring))
    own = jnp.stack(held)
    other = core_swap(own, count)
    core = me % 2
    both = jnp.where(core == 0, jnp.stack([own, other], 1), jnp.stack([other, own], 1))
    if pairs == 2:
        order = jnp.where(me // 2 == 0, both, both[::-1])
    else:
        order = jnp.take(both, (me // 2 - jnp.arange(pairs)) % pairs, axis=0)
    return order.reshape((count,) + block.shape)


def vocab_scatter(blocks, count, wire):
    me = lax.axis_index("vocab")
    pairs = count // 2
    core, row = me % 2, me // 2
    split = blocks.reshape((pairs, 2) + blocks.shape[1:])
    mine = jnp.where(core == 0, split[:, 0], split[:, 1])
    theirs = jnp.where(core == 0, split[:, 1], split[:, 0])
    mine = mine + core_swap(theirs.astype(wire), count).astype(jnp.float32)
    ring = [(i, (i + 2) % count) for i in range(count)]
    total = lax.dynamic_index_in_dim(mine, (row - 1) % pairs, 0, keepdims=False)
    for step in range(1, pairs):
        got = lax.ppermute(total.astype(wire), "vocab", ring).astype(jnp.float32)
        total = got + lax.dynamic_index_in_dim(mine, (row - 1 - step) % pairs, 0, keepdims=False)
    return total


def comp_scatter(z_rows, grad_rows, owners, wire):
    me = lax.axis_index("comp")
    order = list(range(0, owners, 2)) + list(range(1, owners, 2))[::-1]
    place_of = [order.index(i) for i in range(owners)]
    place = jnp.array(place_of, jnp.int32)[me]
    order_array = jnp.array(order, jnp.int32)
    rows = z_rows.shape[1] // owners
    half = rows // 2

    def part(sign, step):
        owner = order_array[(place - sign * (1 + step)) % owners]
        start = owner * rows + (0 if sign == 1 else half)
        block = lax.dynamic_slice_in_dim(z_rows, start, half, 1)
        return lax.dot_general(
            block, grad_rows, (((0,), (0,)), ((), ())), preferred_element_type=jnp.float32
        )

    totals = []
    rings = [
        (sign, [(order[p], order[(p + sign) % owners]) for p in range(owners)]) for sign in (1, -1)
    ]
    totals = [part(sign, 0) for sign, _ in rings]
    for step in range(1, owners):
        moved = [
            lax.ppermute(total.astype(wire), "comp", ring) for total, (_, ring) in zip(totals, rings)
        ]
        totals = [
            got.astype(jnp.float32) + part(sign, step) for got, (sign, _) in zip(moved, rings)
        ]
    return jnp.concatenate(totals, axis=0)


def shards(hidden, routes, targets, saved_lse, target_logprob, prior_weight, projection, embedding):
    highest = lax.Precision.HIGHEST
    tok_dev, model_width = hidden.shape
    top = routes.shape[1]
    comp_dev = projection.shape[0]
    cols = projection.shape[2]
    voc_dev = embedding.shape[1]
    owners = lax.axis_size("comp")
    slices = lax.axis_size("vocab")
    experts_all = comp_dev * owners
    capacity = max(2, (2 * tok_dev * top + experts_all - 1) // experts_all)
    slot_rows = owners * capacity
    comp_index = lax.axis_index("comp")
    vocab_index = lax.axis_index("vocab")
    wire = jnp.bfloat16 if owners <= 8 else jnp.float32

    own_cols = lax.dynamic_slice_in_dim(hidden, vocab_index * cols, cols, 1)
    cols_all = lax.all_gather(own_cols, "comp", axis=0, tiled=True)
    hidden_all = vocab_gather(cols_all, slices)

    partial_logits = jnp.dot(own_cols, prior_weight, preferred_element_type=jnp.float32)
    prior_logits = lax.psum(partial_logits, "vocab")
    comp_ids = jnp.arange(experts_all, dtype=jnp.int32)
    picked = (routes[:, :, None] == comp_ids[None, None, :]).astype(jnp.float32)
    selected = jnp.sum(picked * prior_logits[:, None, :], axis=2)
    gate = jax.nn.softmax(selected, axis=-1)
    posterior = jax.nn.softmax(jax.nn.log_softmax(selected, axis=-1) + target_logprob, axis=-1)
    prior_grads = jnp.sum((gate - posterior)[:, :, None] * picked, axis=1)
    prior_back = lax.dot_general(
        prior_grads, prior_weight.astype(jnp.float32), (((1,), (1,)), ((), ())), precision=highest
    )
    packed = jnp.concatenate(
        [
            posterior,
            saved_lse,
            jnp.repeat(targets.astype(jnp.float32)[:, None], top, axis=1),
            routes.astype(jnp.float32),
            prior_grads,
        ],
        axis=1,
    )
    packed_all = lax.all_gather(packed, "comp", axis=0, tiled=True)
    grad_prior = lax.dot_general(
        cols_all.astype(jnp.float32),
        packed_all[:, 4 * top :],
        (((0,), (0,)), ((), ())),
        precision=highest,
    )

    pairs = tok_dev * top

    def pair_values(index):
        return packed_all[:, index * top : (index + 1) * top].reshape(owners, pairs)

    pair_comp = pair_values(3)
    own_ids = (comp_index * comp_dev + jnp.arange(comp_dev, dtype=jnp.int32)).astype(jnp.float32)
    hit = pair_comp[None, :, :] == own_ids[:, None, None]
    pair_ids = jnp.arange(pairs, dtype=jnp.int32)
    before = (pair_ids[:, None] < pair_ids[None, :]).astype(jnp.bfloat16)
    rank = jnp.einsum(
        "lbp,pq->lbq", hit.astype(jnp.bfloat16), before, preferred_element_type=jnp.float32
    )
    place = jnp.where(hit, rank, -1.0)
    slot_ids = jnp.arange(capacity, dtype=jnp.int32).astype(jnp.float32)
    dispatch = (place[:, :, None, :] == slot_ids[None, None, :, None]).astype(jnp.float32)

    def to_slots(index):
        values = pair_values(index)
        return jnp.sum(dispatch * values[None, :, None, :], axis=3).reshape(comp_dev * slot_rows)

    post_rows, lse_rows = to_slots(0), to_slots(1)
    target_rows = to_slots(2).astype(jnp.int32)
    fold = (pair_ids[:, None] // top == jnp.arange(tok_dev, dtype=jnp.int32)[None, :]).astype(jnp.bfloat16)
    token_hit = jnp.einsum(
        "lbsp,pt->lbst", dispatch.astype(jnp.bfloat16), fold, preferred_element_type=jnp.float32
    ).astype(jnp.bfloat16)

    rows_in = jnp.einsum(
        "lbst,kbtd->lbskd",
        token_hit,
        hidden_all.reshape(slices, owners, tok_dev, cols),
        preferred_element_type=jnp.float32,
    ).astype(jnp.bfloat16).reshape(comp_dev, slot_rows, model_width)
    preact = jnp.einsum("lrd,lde->lre", rows_in, projection, preferred_element_type=jnp.float32)
    tanh_value = jnp.tanh(preact)
    z_local = tanh_value.astype(jnp.bfloat16).reshape(comp_dev * slot_rows, cols)
    z_blocks = vocab_gather(z_local, slices)
    z_all = jnp.swapaxes(z_blocks, 0, 1).reshape(comp_dev * slot_rows, slices * cols)
    logits = jnp.dot(z_all, embedding, preferred_element_type=jnp.float32)
    vocab_ids = vocab_index * voc_dev + jnp.arange(voc_dev, dtype=jnp.int32)
    target_hit = (target_rows[:, None] == vocab_ids[None, :]).astype(jnp.float32)
    logit_grads = (post_rows[:, None] * (jnp.exp(logits - lse_rows[:, None]) - target_hit)).astype(
        jnp.bfloat16
    )
    logit_grads = lax.optimization_barrier(logit_grads)
    feature_parts = jnp.einsum(
        "rv,kdv->krd",
        logit_grads,
        embedding.reshape(slices, cols, voc_dev),
        preferred_element_type=jnp.float32,
    )
    feature_grads = vocab_scatter(feature_parts, slices, wire).reshape(comp_dev, slot_rows, cols)
    pre_grads = (feature_grads * (1.0 - tanh_value * tanh_value)).astype(jnp.bfloat16)
    slot_parts = jnp.einsum(
        "lre,lkde->klrd",
        pre_grads,
        projection.reshape(comp_dev, slices, model_width // slices, cols),
        preferred_element_type=jnp.float32,
    )
    slot_share = vocab_scatter(slot_parts, slices, wire)
    token_parts = jnp.einsum(
        "lbst,lbsd->btd",
        token_hit.astype(jnp.float32),
        slot_share.reshape(comp_dev, owners, capacity, model_width // slices),
        precision=highest,
    )
    returned = lax.all_to_all(
        token_parts.astype(wire), "comp", split_axis=0, concat_axis=0, tiled=True
    )
    grad_hidden = jnp.sum(returned.astype(jnp.float32), axis=0) + prior_back
    grad_projection = jnp.einsum(
        "lrd,lre->lde", rows_in, pre_grads, preferred_element_type=jnp.float32
    ).astype(jnp.bfloat16)
    grad_embedding = comp_scatter(z_all, logit_grads, owners, wire).astype(jnp.bfloat16)
    return (grad_hidden, grad_prior, grad_projection, grad_embedding)


def solution(mesh):
    return jax.shard_map(
        shards,
        mesh=mesh,
        in_specs=(
            P("comp", None),
            P("comp", None),
            P("comp"),
            P("comp", None),
            P("comp", None),
            P("vocab", None),
            P("comp", None, "vocab"),
            P(None, "vocab"),
        ),
        out_specs=(
            P("comp", "vocab"),
            P("vocab", None),
            P("comp", None, "vocab"),
            P("comp", "vocab"),
        ),
        check_vma=False,
    )
```
